32 devices in a mesh: kv: 2 (over x), batch: 16 (over z, y, core).
Axes of the slice: x: 2, y: 2, z: 4, core: 2. Of those that a mesh axis runs over, the one named last changes fastest.
Arguments:
- queries: bfloat16 [64, 32, 128], P(('kv', 'batch')), may hold values from -64 to 64
- prefix_keys: bfloat16 [8192, 8, 128], P('batch', 'kv'), may hold values from -6 to 6
- prefix_values: bfloat16 [8192, 8, 128], P('batch', 'kv'), may hold values from -6 to 6
- suffix_keys: bfloat16 [64, 2048, 8, 128], P('batch', None, 'kv'), may hold values from -6 to 6
- suffix_values: bfloat16 [64, 2048, 8, 128], P('batch', None, 'kv'), may hold values from -6 to 6
- suffix_lengths: int32 [64], P('batch'), may hold values from 512 to 2048, as said below
- slot_sequence: int32 [64], P('batch'), may hold values from 0 to 63, as said below
Outputs:
- attended: bfloat16 [64, 32, 128], P(('kv', 'batch'))
The draws below stay inside these ranges and needn't reach their ends.
Inputs may be any that keep to these rules, and one draw needn't show every extreme that they name: `suffix_lengths`: some slot holds exactly 2048 live tokens. `slot_sequence`: each sequence's suffix occupies exactly one slot; the 64 / 16 slots of one index of batch hold sequences whose output rows lie on pairwise different indices of batch.
All inputs are finite; a program needn't handle non-finite values.
Results may differ from the reference program's by a relative error of at most 0.007.
Values may be sent and summed in bfloat16 or wider, within the bound.
A program may use at most 64 MiB of HBM per device.

```python
import jax
import jax.numpy as jnp
from jax import lax

HEADS = 32
KV_HEADS = 8
HEAD_DIM = 128
SEQ_DEV = 2
PREFIX = 8192
SUFFIX = 2048
BATCH = 64
N_BATCH = 16


def draw_queries(key, part):
    sampled = jnp.clip(2.5 * jax.random.normal(jax.random.fold_in(key, 1), (BATCH, HEADS, HEAD_DIM), jnp.float32), -15.0, 15.0)
    return sampled.astype(jnp.bfloat16)


def draw_prefix_keys(key, part):
    sampled = jnp.clip(jax.random.normal(jax.random.fold_in(key, 2), (PREFIX, KV_HEADS, HEAD_DIM), jnp.float32), -6.0, 6.0)
    return sampled.astype(jnp.bfloat16)


def draw_suffix_keys(key, part):
    sampled = jnp.clip(jax.random.normal(jax.random.fold_in(key, 3), (BATCH, SUFFIX, KV_HEADS, HEAD_DIM), jnp.float32), -6.0, 6.0)
    return sampled.astype(jnp.bfloat16)


def draw_suffix_lengths(key, part):
    drawn = jax.random.randint(jax.random.fold_in(key, 4), (BATCH,), SUFFIX // 4, SUFFIX + 1, jnp.int32)
    longest = jax.random.randint(jax.random.fold_in(key, 5), (), 0, BATCH, jnp.int32)
    return jnp.where(jnp.arange(BATCH) == longest, SUFFIX, drawn).astype(jnp.int32)


def draw_slot_sequence(key, part):
    per_index = BATCH // N_BATCH
    offsets = jax.random.permutation(jax.random.fold_in(key, 21), N_BATCH).astype(jnp.int32)
    shifts = jax.random.permutation(jax.random.fold_in(key, 22), N_BATCH)[:per_index].astype(jnp.int32)
    column = (offsets[:, None] + shifts[None, :]) % N_BATCH
    member_key = jax.random.fold_in(key, 23)
    member_table = jax.vmap(lambda index: jax.random.permutation(jax.random.fold_in(member_key, index), per_index))(jnp.arange(N_BATCH)).astype(jnp.int32)
    ranks = jnp.arange(per_index).astype(jnp.int32)
    member = member_table[column, ranks[None, :]]
    group = member // SEQ_DEV
    within = member % SEQ_DEV
    sequence = (group * N_BATCH + column) * SEQ_DEV + within
    return sequence.reshape(BATCH).astype(jnp.int32)


def level_of(stream_key, shape, cuts, smallest, top_value):
    loudness, own = 1.0, jax.random.fold_in(stream_key, 6)
    for axis_at, blocks in cuts:
        steps = jnp.exp(jax.random.uniform(jax.random.fold_in(own, axis_at), (blocks,), jnp.float32, smallest / len(cuts), top_value / len(cuts)))
        loudness = loudness * jnp.repeat(steps, shape[axis_at] // blocks).reshape([-1 if axis == axis_at else 1 for axis in range(len(shape))])
    return loudness


def centred(rng, dims, spread, reach, cuts=(), dtype=jnp.bfloat16):
    values = spread * jax.random.normal(rng, dims, jnp.float32)
    if cuts:
        values = values * level_of(rng, dims, cuts, -0.22, 0.18)
    return jnp.clip(values, -reach, reach).astype(dtype)


def setup_inputs(seed: int = 0) -> dict:
    arg_keys = jax.random.split(jax.random.key(seed), 8)
    queries = draw_queries(jax.random.fold_in(arg_keys[7], 71), 0)
    prefix_keys = draw_prefix_keys(jax.random.fold_in(arg_keys[7], 71), 0)
    prefix_values = centred(arg_keys[2], (PREFIX, KV_HEADS, HEAD_DIM), 1.0, 6.0, ((0, 16), (1, 2)))
    suffix_keys = draw_suffix_keys(jax.random.fold_in(arg_keys[7], 71), 0)
    suffix_values = centred(arg_keys[4], (BATCH, SUFFIX, KV_HEADS, HEAD_DIM), 1.0, 6.0, ((0, 16), (2, 2)))
    suffix_lengths = draw_suffix_lengths(jax.random.fold_in(arg_keys[7], 71), 0)
    slot_sequence = draw_slot_sequence(jax.random.fold_in(arg_keys[7], 71), 0)
    return {"queries": queries, "prefix_keys": prefix_keys, "prefix_values": prefix_values, "suffix_keys": suffix_keys, "suffix_values": suffix_values, "suffix_lengths": suffix_lengths, "slot_sequence": slot_sequence}


negative_fill = -1e30


def reference(queries, prefix_keys, prefix_values, suffix_keys, suffix_values, suffix_lengths, slot_sequence):
    group_size = HEADS // KV_HEADS
    scale = HEAD_DIM ** -0.5
    grouped = queries.reshape(BATCH, KV_HEADS, group_size, HEAD_DIM).transpose(1, 0, 2, 3)

    def prefix_head(operands):
        query_head, key_head, value_head = operands
        scores = jnp.einsum("bjd,td->bjt", query_head.astype(jnp.float32), key_head.astype(jnp.float32)) * scale
        best = jnp.max(scores, axis=-1)
        weights = jnp.exp(scores - best[..., None])
        total = jnp.sum(weights, axis=-1)
        rounded = lax.optimization_barrier(weights.astype(jnp.bfloat16))
        accum = jnp.einsum("bjt,td->bjd", rounded.astype(jnp.float32), value_head.astype(jnp.float32))
        return best, total, accum

    pre_best, pre_total, pre_acc = lax.map(prefix_head, (grouped, prefix_keys.transpose(1, 0, 2), prefix_values.transpose(1, 0, 2)))
    pre_best = pre_best.transpose(1, 0, 2).reshape(BATCH, HEADS)
    pre_total = pre_total.transpose(1, 0, 2).reshape(BATCH, HEADS)
    pre_acc = pre_acc.transpose(1, 0, 2, 3).reshape(BATCH, HEADS, HEAD_DIM)

    slot_queries = queries[slot_sequence].reshape(BATCH, KV_HEADS, group_size, HEAD_DIM)
    position = jnp.arange(SUFFIX).astype(jnp.int32)

    def suffix_slot(operands):
        query_slot, key_slot, value_slot, length = operands
        scores = jnp.einsum("kjd,tkd->kjt", query_slot.astype(jnp.float32), key_slot.astype(jnp.float32)) * scale
        scores = jnp.where(position[None, None, :] < length, scores, negative_fill)
        best = jnp.max(scores, axis=-1)
        weights = jnp.exp(scores - best[..., None])
        total = jnp.sum(weights, axis=-1)
        rounded = lax.optimization_barrier(weights.astype(jnp.bfloat16))
        accum = jnp.einsum("kjt,tkd->kjd", rounded.astype(jnp.float32), value_slot.astype(jnp.float32))
        return best, total, accum

    suf_best, suf_total, suf_acc = lax.map(suffix_slot, (slot_queries, suffix_keys, suffix_values, suffix_lengths))
    seq_best = jnp.zeros((BATCH, HEADS), jnp.float32).at[slot_sequence].set(suf_best.reshape(BATCH, HEADS))
    seq_total = jnp.zeros((BATCH, HEADS), jnp.float32).at[slot_sequence].set(suf_total.reshape(BATCH, HEADS))
    seq_acc = jnp.zeros((BATCH, HEADS, HEAD_DIM), jnp.float32).at[slot_sequence].set(suf_acc.reshape(BATCH, HEADS, HEAD_DIM))
    top = jnp.maximum(pre_best, seq_best)
    first = jnp.exp(pre_best - top)
    second = jnp.exp(seq_best - top)
    numerator = pre_acc * first[..., None] + seq_acc * second[..., None]
    denominator = pre_total * first + seq_total * second
    return (numerator / denominator[..., None]).astype(jnp.bfloat16)
```

```python
import functools

import jax
import jax.numpy as jnp
from jax import lax
from jax.experimental import pallas as pl
from jax.experimental.pallas import tpu as pltpu
from jax.sharding import PartitionSpec as P

MESH = pl.DeviceIdType.MESH
FILL = -1e30
F32 = jnp.float32
BF16 = jnp.bfloat16


def kernel(
    kv_count,
    batch_count,
    group,
    scale,
    seq_ref,
    len_ref,
    q_ref,
    pk_hbm,
    pv_hbm,
    sk_hbm,
    sv_hbm,
    out_ref,
    pk_raw,
    pv_raw,
    sk,
    sv,
    spread,
    pk,
    pv,
    qbuf,
    qf,
    acc,
    best,
    total,
    suf_acc,
    suf_best,
    suf_total,
    send_acc,
    send_stat,
    recv_acc,
    recv_stat,
    weight,
    pre_sem,
    suf_sem,
    q_send,
    q_recv,
    a_send,
    a_recv,
    s_send,
    s_recv,
):
    devices = kv_count * batch_count
    per_device, heads, dim = q_ref.shape
    local = heads // kv_count
    kv_local = local // group
    sequences = devices * per_device
    slots, rows, _ = sk_hbm.shape
    prefix_rows = pk_hbm.shape[0]
    prefix = prefix_rows // kv_local

    my_kv = lax.axis_index("kv")
    my_batch = lax.axis_index("batch")
    me = my_kv * batch_count + my_batch

    pre_copies = [
        pltpu.make_async_copy(pk_hbm, pk_raw, pre_sem.at[0]),
        pltpu.make_async_copy(pv_hbm, pv_raw, pre_sem.at[1]),
    ]
    for copy in pre_copies:
        copy.start()

    def suffix_copies(slot):
        return (
            pltpu.make_async_copy(sk_hbm.at[slot], sk.at[slot], suf_sem.at[0, slot]),
            pltpu.make_async_copy(sv_hbm.at[slot], sv.at[slot], suf_sem.at[1, slot]),
        )

    for slot in range(slots):
        for copy in suffix_copies(slot):
            copy.start()

    barrier = pltpu.get_barrier_semaphore()

    def peer(step):
        other = lax.rem(me + step, devices)
        return other, (other // batch_count, lax.rem(other, batch_count))

    def greet(step, carry):
        _, place = peer(step)
        pl.semaphore_signal(barrier, inc=1, device_id=place, device_id_type=MESH)
        return carry

    lax.fori_loop(1, devices, greet, 0)
    pl.semaphore_wait(barrier, devices - 1)

    def query_copy(step):
        other, place = peer(step)
        heads_there = pl.ds(pl.multiple_of(place[0] * local, local), local)
        return pltpu.make_async_remote_copy(
            src_ref=q_ref.at[:, heads_there, :],
            dst_ref=qbuf.at[pl.ds(me * per_device, per_device)],
            send_sem=q_send.at[other],
            recv_sem=q_recv.at[me],
            device_id=place,
            device_id_type=MESH,
        )

    def query_arrival(step):
        other, place = peer(step)
        return pltpu.make_async_remote_copy(
            src_ref=q_ref.at[:, pl.ds(0, local), :],
            dst_ref=qbuf.at[pl.ds(other * per_device, per_device)],
            send_sem=q_send.at[other],
            recv_sem=q_recv.at[other],
            device_id=place,
            device_id_type=MESH,
        )

    def query_start(step, carry):
        query_copy(step).start()
        return carry

    lax.fori_loop(1, devices, query_start, 0)
    my_heads = pl.ds(pl.multiple_of(my_kv * local, local), local)
    qbuf[pl.ds(me * per_device, per_device)] = q_ref[:, my_heads, :]

    for copy, raw, parted in zip(pre_copies, (pk_raw, pv_raw), (pk, pv)):
        copy.wait()
        spread[...] = raw[...].astype(F32)
        for k in range(kv_local):
            parted[k] = spread[pl.ds(k, prefix, stride=kv_local), :].astype(BF16)

    def query_wait(step, carry):
        query_arrival(step).wait()
        return carry

    lax.fori_loop(1, devices, query_wait, 0)

    qf[...] = qbuf[...].astype(F32).reshape(sequences * local, dim)
    contract_last = (((1,), (1,)), ((), ()))
    for k in range(kv_local):
        parts = [qf[pl.ds(k * group + j, sequences, stride=local), :] for j in range(group)]
        q = jnp.concatenate(parts, axis=0).astype(BF16)
        scores = lax.dot_general(q, pk[k], contract_last, preferred_element_type=F32) * scale
        row_best = jnp.max(scores, axis=-1, keepdims=True)
        weights = jnp.exp(scores - row_best)
        row_total = jnp.sum(weights, axis=-1, keepdims=True)
        row_acc = jnp.dot(weights.astype(BF16), pv[k], preferred_element_type=F32)
        wide_best = jnp.broadcast_to(row_best, row_acc.shape)
        wide_total = jnp.broadcast_to(row_total, row_acc.shape)
        for j in range(group):
            there = pl.ds(k * group + j, sequences, stride=local)
            here = slice(j * sequences, (j + 1) * sequences)
            acc[there, :] = row_acc[here]
            best[there, :] = wide_best[here]
            total[there, :] = wide_total[here]

    column = lax.broadcasted_iota(jnp.int32, (local, rows), 1)
    head_row = lax.broadcasted_iota(jnp.int32, (local, rows), 0)
    own_head = lax.rem(column, kv_local) == head_row // group
    for slot in range(slots):
        for copy in suffix_copies(slot):
            copy.wait()
        q = qbuf[seq_ref[slot]]
        scores = lax.dot_general(q, sk[slot], contract_last, preferred_element_type=F32) * scale
        live = own_head & (column < len_ref[slot] * kv_local)
        scores = jnp.where(live, scores, FILL)
        row_best = jnp.max(scores, axis=-1, keepdims=True)
        weights = jnp.exp(scores - row_best)
        row_total = jnp.sum(weights, axis=-1, keepdims=True)
        suf_acc[slot] = jnp.dot(weights.astype(BF16), sv[slot], preferred_element_type=F32)
        suf_best[slot] = jnp.broadcast_to(row_best, (local, dim))
        suf_total[slot] = jnp.broadcast_to(row_total, (local, dim))

    lane = lax.broadcasted_iota(jnp.int32, (local, dim), 1)
    sub = lax.broadcasted_iota(jnp.int32, (local, dim), 0)
    half = per_device * local

    def merged(other):
        accs = []
        stat = jnp.zeros((local, dim), F32)
        for w in range(per_device):
            sequence = other * per_device + w
            at = jnp.int32(0)
            hit = jnp.int32(0)
            for slot in range(slots):
                same = (seq_ref[slot] == sequence).astype(jnp.int32)
                at = jnp.maximum(at, same * slot)
                hit = jnp.maximum(hit, same)
            table = pl.ds(pl.multiple_of(sequence * local, local), local)
            first_best = best[table, :]
            second_best = jnp.where(hit > 0, suf_best[at], FILL)
            new_best = jnp.maximum(first_best, second_best)
            first = jnp.exp(first_best - new_best)
            second = jnp.where(hit > 0, jnp.exp(second_best - new_best), 0.0)
            new_total = total[table, :] * first + suf_total[at] * second
            accs.append((acc[table, :] * first + suf_acc[at] * second).astype(BF16))
            stat = jnp.where(lane == sub + w * local, new_best, stat)
            stat = jnp.where(lane == sub + half + w * local, new_total, stat)
        return accs, jnp.sum(stat, axis=0, keepdims=True)

    def result_copies(step):
        other, place = peer(step)
        return (
            pltpu.make_async_remote_copy(
                src_ref=send_acc.at[other],
                dst_ref=recv_acc.at[me],
                send_sem=a_send.at[other],
                recv_sem=a_recv.at[me],
                device_id=place,
                device_id_type=MESH,
            ),
            pltpu.make_async_remote_copy(
                src_ref=send_stat.at[other],
                dst_ref=recv_stat.at[me],
                send_sem=s_send.at[other],
                recv_sem=s_recv.at[me],
                device_id=place,
                device_id_type=MESH,
            ),
        )

    def result_arrivals(step):
        other, place = peer(step)
        return (
            pltpu.make_async_remote_copy(
                src_ref=send_acc.at[other],
                dst_ref=recv_acc.at[other],
                send_sem=a_send.at[other],
                recv_sem=a_recv.at[other],
                device_id=place,
                device_id_type=MESH,
            ),
            pltpu.make_async_remote_copy(
                src_ref=send_stat.at[other],
                dst_ref=recv_stat.at[other],
                send_sem=s_send.at[other],
                recv_sem=s_recv.at[other],
                device_id=place,
                device_id_type=MESH,
            ),
        )

    def result_start(step, carry):
        other, _ = peer(step)
        accs, stat = merged(other)
        for w in range(per_device):
            send_acc[other, w] = accs[w]
        send_stat[other] = stat
        for copy in result_copies(step):
            copy.start()
        return carry

    lax.fori_loop(1, devices, result_start, 0)
    accs, stat = merged(me)
    for w in range(per_device):
        recv_acc[me, w] = accs[w]
    recv_stat[me] = stat

    def result_wait(step, carry):
        for copy in result_arrivals(step):
            copy.wait()
        return carry

    lax.fori_loop(1, devices, result_wait, 0)

    for g in range(kv_count):
        own = slice(g * batch_count, (g + 1) * batch_count)
        stats = recv_stat[own, 0, :]
        part_best = stats[:, :half]
        part_total = stats[:, half : 2 * half]
        top = jnp.max(part_best, axis=0, keepdims=True)
        factor = jnp.exp(part_best - top)
        denominator = jnp.sum(part_total * factor, axis=0, keepdims=True)
        weight[own, 0, :] = jnp.concatenate(
            [factor / denominator, jnp.zeros((batch_count, dim - half), F32)], axis=1
        )

        def add(index, sums):
            source = g * batch_count + index
            row = weight[source]
            new = []
            for w in range(per_device):
                picked = jnp.where(lane == sub + w * local, row, 0.0)
                share = jnp.sum(picked, axis=-1, keepdims=True)
                new.append(sums[w] + share * recv_acc[source, w].astype(F32))
            return tuple(new)

        start = tuple(jnp.zeros((local, dim), F32) for _ in range(per_device))
        sums = lax.fori_loop(0, batch_count, add, start, unroll=4)
        for w in range(per_device):
            out_ref[w, g * local : (g + 1) * local, :] = sums[w].astype(BF16)


def solution(mesh):
    kv_count = mesh.shape["kv"]
    batch_count = mesh.shape["batch"]
    devices = kv_count * batch_count

    def step(queries, prefix_keys, prefix_values, suffix_keys, suffix_values, lengths, slot_sequence):
        per_device, heads, dim = queries.shape
        local = heads // kv_count
        prefix, kv_local, _ = prefix_keys.shape
        slots, suffix, _, _ = suffix_keys.shape
        group = local // kv_local
        sequences = devices * per_device
        flat = sequences * local
        vmem = pl.BlockSpec(memory_space=pltpu.VMEM)
        smem = pl.BlockSpec(memory_space=pltpu.SMEM)
        hbm = pl.BlockSpec(memory_space=pl.ANY)
        dma = pltpu.SemaphoreType.DMA
        return pl.pallas_call(
            functools.partial(kernel, kv_count, batch_count, group, dim ** (-0.5)),
            out_shape=jax.ShapeDtypeStruct(queries.shape, BF16),
            in_specs=[smem, smem, vmem, hbm, hbm, hbm, hbm],
            out_specs=vmem,
            scratch_shapes=[
                pltpu.VMEM((prefix * kv_local, dim), BF16),
                pltpu.VMEM((prefix * kv_local, dim), BF16),
                pltpu.VMEM((slots, suffix * kv_local, dim), BF16),
                pltpu.VMEM((slots, suffix * kv_local, dim), BF16),
                pltpu.VMEM((prefix * kv_local, dim), F32),
                pltpu.VMEM((kv_local, prefix, dim), BF16),
                pltpu.VMEM((kv_local, prefix, dim), BF16),
                pltpu.VMEM((sequences, local, dim), BF16),
                pltpu.VMEM((flat, dim), F32),
                pltpu.VMEM((flat, dim), F32),
                pltpu.VMEM((flat, dim), F32),
                pltpu.VMEM((flat, dim), F32),
                pltpu.VMEM((slots, local, dim), F32),
                pltpu.VMEM((slots, local, dim), F32),
                pltpu.VMEM((slots, local, dim), F32),
                pltpu.VMEM((devices, per_device, local, dim), BF16),
                pltpu.VMEM((devices, 1, dim), F32),
                pltpu.VMEM((devices, per_device, local, dim), BF16),
                pltpu.VMEM((devices, 1, dim), F32),
                pltpu.VMEM((devices, 1, dim), F32),
                dma((2,)),
                dma((2, slots)),
                dma((devices,)),
                dma((devices,)),
                dma((devices,)),
                dma((devices,)),
                dma((devices,)),
                dma((devices,)),
            ],
            compiler_params=pltpu.CompilerParams(
                collective_id=0, has_side_effects=True, vmem_limit_bytes=60 * 1024 * 1024
            ),
        )(
            slot_sequence,
            lengths,
            queries,
            prefix_keys.reshape(prefix * kv_local, dim),
            prefix_values.reshape(prefix * kv_local, dim),
            suffix_keys.reshape(slots, suffix * kv_local, dim),
            suffix_values.reshape(slots, suffix * kv_local, dim),
        )

    return jax.shard_map(
        step,
        mesh=mesh,
        in_specs=(
            P(("kv", "batch"), None, None),
            P("batch", "kv", None),
            P("batch", "kv", None),
            P("batch", None, "kv", None),
            P("batch", None, "kv", None),
            P("batch"),
            P("batch"),
        ),
        out_specs=P(("kv", "batch"), None, None),
        check_vma=False,
    )
```

```python
import functools

import jax
import jax.numpy as jnp
from jax import lax
from jax.experimental import pallas as pl
from jax.experimental.pallas import tpu as pltpu
from jax.sharding import PartitionSpec as P

MESH = pl.DeviceIdType.MESH
FILL = -1e30
F32 = jnp.float32
BF16 = jnp.bfloat16


def kernel(
    kv_count,
    batch_count,
    group,
    scale,
    seq_ref,
    len_ref,
    q_ref,
    pk_hbm,
    pv_hbm,
    sk_hbm,
    sv_hbm,
    out_ref,
    pk_raw,
    pv_raw,
    sk,
    sv,
    spread,
    pk,
    pv,
    qbuf,
    qf,
    acc,
    best,
    total,
    mate_acc,
    mate_best,
    mate_total,
    suf_acc,
    suf_best,
    suf_total,
    send_acc,
    send_stat,
    recv_acc,
    recv_stat,
    send_suf,
    send_sufstat,
    recv_suf,
    recv_sufstat,
    weight,
    pre_sem,
    suf_sem,
    q_send,
    q_recv,
    f_send,
    f_recv,
    m_send,
    m_recv,
    r_send,
    r_recv,
    u_send,
    u_recv,
):
    devices = kv_count * batch_count
    per_device, heads, dim = q_ref.shape
    local = heads // kv_count
    kv_local = local // group
    slots, rows, _ = sk_hbm.shape
    prefix_rows = pk_hbm.shape[0]
    prefix = prefix_rows // kv_local

    my_kv = lax.axis_index("kv")
    my_batch = lax.axis_index("batch")
    me = my_kv * batch_count + my_batch
    pairs = devices // 2
    core = lax.rem(me, 2)
    far = 1 - core
    my_pair = me // 2
    mate_place = (my_kv, my_batch + 1 - 2 * core)
    pair_rows = pairs * per_device

    pre_copies = [
        pltpu.make_async_copy(pk_hbm, pk_raw, pre_sem.at[0]),
        pltpu.make_async_copy(pv_hbm, pv_raw, pre_sem.at[1]),
    ]
    for copy in pre_copies:
        copy.start()

    def suffix_copies(slot):
        return (
            pltpu.make_async_copy(sk_hbm.at[slot], sk.at[slot], suf_sem.at[0, slot]),
            pltpu.make_async_copy(sv_hbm.at[slot], sv.at[slot], suf_sem.at[1, slot]),
        )

    for slot in range(slots):
        for copy in suffix_copies(slot):
            copy.start()

    barrier = pltpu.get_barrier_semaphore()

    def peer(step):
        other = lax.rem(me + step, devices)
        return other, (other // batch_count, lax.rem(other, batch_count))

    def greet(step, carry):
        _, place = peer(step)
        pl.semaphore_signal(barrier, inc=1, device_id=place, device_id_type=MESH)
        return carry

    lax.fori_loop(1, devices, greet, 0)
    pl.semaphore_wait(barrier, devices - 1)

    def send(src, dst, send_sem, recv_sem, place):
        return pltpu.make_async_remote_copy(
            src_ref=src,
            dst_ref=dst,
            send_sem=send_sem,
            recv_sem=recv_sem,
            device_id=place,
            device_id_type=MESH,
        )

    my_heads = pl.ds(pl.multiple_of(my_kv * local, local), local)

    def query_start(step, carry):
        other, place = peer(2 * step)
        heads_there = pl.ds(pl.multiple_of(place[0] * local, local), local)
        send(
            q_ref.at[:, heads_there, :], qbuf.at[my_pair, core], q_send.at[other // 2],
            q_recv.at[my_pair], place,
        ).start()
        return carry

    lax.fori_loop(1, pairs, query_start, 0)
    own_forward = send(
        q_ref.at[:, my_heads, :], qbuf.at[my_pair, core], f_send.at[my_pair], f_recv.at[my_pair],
        mate_place,
    )
    own_forward.start()
    qbuf[my_pair, core] = q_ref[:, my_heads, :]

    for copy, raw, parted in zip(pre_copies, (pk_raw, pv_raw), (pk, pv)):
        copy.wait()
        spread[...] = raw[...].astype(F32)
        for k in range(kv_local):
            parted[k] = spread[pl.ds(k, prefix, stride=kv_local), :].astype(BF16)

    def forward(pair):
        return send(
            qbuf.at[pair, core], qbuf.at[pair, core], f_send.at[pair], f_recv.at[pair], mate_place
        )

    def query_wait(step, carry):
        other, place = peer(2 * step)
        pair = other // 2
        arrived = qbuf.at[pair, core]
        send(arrived, arrived, q_send.at[pair], q_recv.at[pair], place).wait()
        forward(pair).start()
        return carry

    lax.fori_loop(1, pairs, query_wait, 0)

    contract_last = (((1,), (1,)), ((), ()))

    def attend_prefix(side):
        qf[...] = qbuf[:, side].astype(F32).reshape(pair_rows * local, dim)
        for k in range(kv_local):
            parts = [qf[pl.ds(k * group + j, pair_rows, stride=local), :] for j in range(group)]
            q = jnp.concatenate(parts, axis=0).astype(BF16)
            scores = lax.dot_general(q, pk[k], contract_last, preferred_element_type=F32) * scale
            row_best = jnp.max(scores, axis=-1, keepdims=True)
            weights = jnp.exp(scores - row_best)
            row_total = jnp.sum(weights, axis=-1, keepdims=True)
            row_acc = jnp.dot(weights.astype(BF16), pv[k], preferred_element_type=F32)
            wide_best = jnp.broadcast_to(row_best, row_acc.shape)
            wide_total = jnp.broadcast_to(row_total, row_acc.shape)
            for j in range(group):
                there = pl.ds(k * group + j, pair_rows, stride=local)
                here = slice(j * pair_rows, (j + 1) * pair_rows)
                acc[side, there, :] = row_acc[here]
                best[side, there, :] = wide_best[here]
                total[side, there, :] = wide_total[here]

    attend_prefix(core)

    def forward_wait(pair, carry):
        arrived = qbuf.at[pair, far]
        send(arrived, arrived, f_send.at[pair], f_recv.at[pair], mate_place).wait()
        return carry

    lax.fori_loop(0, pairs, forward_wait, 0)
    attend_prefix(far)

    mate_copies = [
        send(table.at[far], there, m_send.at[n], m_recv.at[n], mate_place)
        for n, (table, there) in enumerate(
            ((acc, mate_acc), (best, mate_best), (total, mate_total))
        )
    ]
    for copy in mate_copies:
        copy.start()

    column = lax.broadcasted_iota(jnp.int32, (local, rows), 1)
    head_row = lax.broadcasted_iota(jnp.int32, (local, rows), 0)
    own_head = lax.rem(column, kv_local) == head_row // group
    lane = lax.broadcasted_iota(jnp.int32, (local, dim), 1)
    sub = lax.broadcasted_iota(jnp.int32, (local, dim), 0)
    half = per_device * local

    def attend_suffix(slot):
        for copy in suffix_copies(slot):
            copy.wait()
        sequence = seq_ref[slot]
        owner = sequence // per_device
        q = qbuf[owner // 2, lax.rem(owner, 2), lax.rem(sequence, per_device)]
        scores = lax.dot_general(q, sk[slot], contract_last, preferred_element_type=F32) * scale
        live = own_head & (column < len_ref[slot] * kv_local)
        scores = jnp.where(live, scores, FILL)
        row_best = jnp.max(scores, axis=-1, keepdims=True)
        weights = jnp.exp(scores - row_best)
        row_total = jnp.sum(weights, axis=-1, keepdims=True)
        suf_acc[slot] = jnp.dot(weights.astype(BF16), sv[slot], preferred_element_type=F32)
        suf_best[slot] = jnp.broadcast_to(row_best, (local, dim))
        suf_total[slot] = jnp.broadcast_to(row_total, (local, dim))

    def mark(stat, w, new_best, new_total):
        stat = jnp.where(lane == sub + w * local, new_best, stat)
        return jnp.where(lane == sub + half + w * local, new_total, stat)

    def fold_pair(pair, acc_out, stat_out):
        stat = jnp.zeros((local, dim), F32)
        for w in range(per_device):
            table = pl.ds(pl.multiple_of((pair * per_device + w) * local, local), local)
            first_best = best[core, table, :]
            second_best = mate_best[table, :]
            new_best = jnp.maximum(first_best, second_best)
            first = jnp.exp(first_best - new_best)
            second = jnp.exp(second_best - new_best)
            new_total = total[core, table, :] * first + mate_total[table, :] * second
            new_acc = acc[core, table, :] * first + mate_acc[table, :] * second
            acc_out[w] = new_acc.astype(BF16)
            stat = mark(stat, w, new_best, new_total)
        stat_out[...] = jnp.sum(stat, axis=0, keepdims=True)

    def prefix_sends(step):
        other, place = peer(2 * step)
        pair = other // 2
        return pair, (
            send(send_acc.at[pair], recv_acc.at[my_pair], r_send.at[0, pair], r_recv.at[0, my_pair], place),
            send(send_stat.at[pair], recv_stat.at[my_pair], r_send.at[1, pair], r_recv.at[1, my_pair], place),
        )

    def prefix_start(step, carry):
        pair, copies = prefix_sends(step)
        fold_pair(pair, send_acc.at[pair], send_stat.at[pair])
        for copy in copies:
            copy.start()
        return carry

    def prefix_wait(step, carry):
        other, place = peer(2 * step)
        pair = other // 2
        send(send_acc.at[pair], recv_acc.at[pair], r_send.at[0, pair], r_recv.at[0, pair], place).wait()
        send(send_stat.at[pair], recv_stat.at[pair], r_send.at[1, pair], r_recv.at[1, pair], place).wait()
        return carry

    def pick_slot(other, acc_out, stat_out):
        at = jnp.int32(0)
        hits = []
        for w in range(per_device):
            hit = jnp.int32(0)
            for slot in range(slots):
                same = (seq_ref[slot] == other * per_device + w).astype(jnp.int32)
                at = jnp.maximum(at, same * slot)
                hit = jnp.maximum(hit, same)
            hits.append(hit)
        stat = jnp.zeros((local, dim), F32)
        for w in range(per_device):
            stat = mark(
                stat, w, jnp.where(hits[w] > 0, suf_best[at], FILL),
                jnp.where(hits[w] > 0, suf_total[at], 0.0),
            )
        acc_out[...] = suf_acc[at].astype(BF16)
        stat_out[...] = jnp.sum(stat, axis=0, keepdims=True)

    def suffix_start(step, carry):
        other, place = peer(step)
        pick_slot(other, send_suf.at[other], send_sufstat.at[other])
        send(send_suf.at[other], recv_suf.at[me], u_send.at[0, other], u_recv.at[0, me], place).start()
        send(send_sufstat.at[other], recv_sufstat.at[me], u_send.at[1, other], u_recv.at[1, me], place).start()
        return carry

    def suffix_wait(step, carry):
        other, place = peer(step)
        send(send_suf.at[other], recv_suf.at[other], u_send.at[0, other], u_recv.at[0, other], place).wait()
        send(send_sufstat.at[other], recv_sufstat.at[other], u_send.at[1, other], u_recv.at[1, other], place).wait()
        return carry

    early = slots // 2
    for slot in range(early):
        attend_suffix(slot)
    for copy in mate_copies:
        copy.wait()
    lax.fori_loop(1, pairs, prefix_start, 0)
    fold_pair(my_pair, recv_acc.at[my_pair], recv_stat.at[my_pair])
    for slot in range(early, slots):
        attend_suffix(slot)
    lax.fori_loop(1, devices, suffix_start, 0)
    pick_slot(me, recv_suf.at[me], recv_sufstat.at[me])
    lax.fori_loop(1, pairs, prefix_wait, 0)

    def column_of(row, w):
        picked = jnp.where(lane == sub + w * local, row, 0.0)
        return jnp.sum(picked, axis=-1, keepdims=True)

    def widen(values):
        return jnp.concatenate([values, jnp.zeros((values.shape[0], dim - half), F32)], axis=1)

    chips = batch_count // 2
    states = []
    for g in range(kv_count):
        stats = recv_stat[g * chips : (g + 1) * chips, 0, :]
        top = jnp.max(stats[:, :half], axis=0, keepdims=True)
        factor = jnp.exp(stats[:, :half] - top)
        denominator = jnp.sum(stats[:, half : 2 * half] * factor, axis=0, keepdims=True)
        weight[:chips, 0, :] = widen(factor)

        def add_prefix(index, sums, g=g):
            row = weight[index]
            return tuple(
                sums[w] + column_of(row, w) * recv_acc[g * chips + index, w].astype(F32)
                for w in range(per_device)
            )

        zeros = tuple(jnp.zeros((local, dim), F32) for _ in range(per_device))
        states.append((top, denominator, lax.fori_loop(0, chips, add_prefix, zeros, unroll=4)))

    lax.fori_loop(1, devices, suffix_wait, 0)
    for g in range(kv_count):
        top, denominator, sums = states[g]
        stats = recv_sufstat[g * batch_count : (g + 1) * batch_count, 0, :]
        new_top = jnp.maximum(top, jnp.max(stats[:, :half], axis=0, keepdims=True))
        factor = jnp.exp(stats[:, :half] - new_top)
        kept = jnp.exp(top - new_top)
        denominator = denominator * kept + jnp.sum(
            stats[:, half : 2 * half] * factor, axis=0, keepdims=True
        )
        weight[:batch_count, 0, :] = widen(factor / denominator)
        kept_row = widen(kept / denominator)
        sums = tuple(sums[w] * column_of(kept_row, w) for w in range(per_device))

        def add_suffix(index, sums, g=g):
            row = weight[index]
            part = recv_suf[g * batch_count + index].astype(F32)
            return tuple(sums[w] + column_of(row, w) * part for w in range(per_device))

        sums = lax.fori_loop(0, batch_count, add_suffix, sums, unroll=4)
        for w in range(per_device):
            out_ref[w, g * local : (g + 1) * local, :] = sums[w].astype(BF16)


def solution(mesh):
    kv_count = mesh.shape["kv"]
    batch_count = mesh.shape["batch"]
    devices = kv_count * batch_count

    def step(queries, prefix_keys, prefix_values, suffix_keys, suffix_values, lengths, slot_sequence):
        per_device, heads, dim = queries.shape
        local = heads // kv_count
        prefix, kv_local, _ = prefix_keys.shape
        slots, suffix, _, _ = suffix_keys.shape
        group = local // kv_local
        sequences = devices * per_device
        flat = sequences * local
        vmem = pl.BlockSpec(memory_space=pltpu.VMEM)
        smem = pl.BlockSpec(memory_space=pltpu.SMEM)
        hbm = pl.BlockSpec(memory_space=pl.ANY)
        dma = pltpu.SemaphoreType.DMA
        return pl.pallas_call(
            functools.partial(kernel, kv_count, batch_count, group, dim ** (-0.5)),
            out_shape=jax.ShapeDtypeStruct(queries.shape, BF16),
            in_specs=[smem, smem, vmem, hbm, hbm, hbm, hbm],
            out_specs=vmem,
            scratch_shapes=[
                pltpu.VMEM((prefix * kv_local, dim), BF16),
                pltpu.VMEM((prefix * kv_local, dim), BF16),
                pltpu.VMEM((slots, suffix * kv_local, dim), BF16),
                pltpu.VMEM((slots, suffix * kv_local, dim), BF16),
                pltpu.VMEM((prefix * kv_local, dim), F32),
                pltpu.VMEM((kv_local, prefix, dim), BF16),
                pltpu.VMEM((kv_local, prefix, dim), BF16),
                pltpu.VMEM((devices // 2, 2, per_device, local, dim), BF16),
                pltpu.VMEM((flat // 2, dim), F32),
                pltpu.VMEM((2, flat // 2, dim), F32),
                pltpu.VMEM((2, flat // 2, dim), F32),
                pltpu.VMEM((2, flat // 2, dim), F32),
                pltpu.VMEM((flat // 2, dim), F32),
                pltpu.VMEM((flat // 2, dim), F32),
                pltpu.VMEM((flat // 2, dim), F32),
                pltpu.VMEM((slots, local, dim), F32),
                pltpu.VMEM((slots, local, dim), F32),
                pltpu.VMEM((slots, local, dim), F32),
                pltpu.VMEM((devices // 2, per_device, local, dim), BF16),
                pltpu.VMEM((devices // 2, 1, dim), F32),
                pltpu.VMEM((devices // 2, per_device, local, dim), BF16),
                pltpu.VMEM((devices // 2, 1, dim), F32),
                pltpu.VMEM((devices, local, dim), BF16),
                pltpu.VMEM((devices, 1, dim), F32),
                pltpu.VMEM((devices, local, dim), BF16),
                pltpu.VMEM((devices, 1, dim), F32),
                pltpu.VMEM((devices, 1, dim), F32),
                dma((2,)),
                dma((2, slots)),
                dma((devices // 2,)),
                dma((devices // 2,)),
                dma((devices // 2,)),
                dma((devices // 2,)),
                dma((3,)),
                dma((3,)),
                dma((2, devices // 2)),
                dma((2, devices // 2)),
                dma((2, devices)),
                dma((2, devices)),
            ],
            compiler_params=pltpu.CompilerParams(
                collective_id=0, has_side_effects=True, vmem_limit_bytes=60 * 1024 * 1024
            ),
        )(
            slot_sequence,
            lengths,
            queries,
            prefix_keys.reshape(prefix * kv_local, dim),
            prefix_values.reshape(prefix * kv_local, dim),
            suffix_keys.reshape(slots, suffix * kv_local, dim),
            suffix_values.reshape(slots, suffix * kv_local, dim),
        )

    return jax.shard_map(
        step,
        mesh=mesh,
        in_specs=(
            P(("kv", "batch"), None, None),
            P("batch", "kv", None),
            P("batch", "kv", None),
            P("batch", None, "kv", None),
            P("batch", None, "kv", None),
            P("batch"),
            P("batch"),
        ),
        out_specs=P(("kv", "batch"), None, None),
        check_vma=False,
    )
```

```python
import functools

import jax
import jax.numpy as jnp
from jax import lax
from jax.experimental import pallas as pl
from jax.experimental.pallas import tpu as pltpu
from jax.sharding import PartitionSpec as P

MESH = pl.DeviceIdType.MESH
FILL = -1e30
F32 = jnp.float32
BF16 = jnp.bfloat16


def kernel(
    kv_count,
    batch_count,
    group,
    scale,
    seq_ref,
    len_ref,
    q_ref,
    pk_hbm,
    pv_hbm,
    sk_hbm,
    sv_hbm,
    out_ref,
    pk_raw,
    pv_raw,
    sk,
    sv,
    spread,
    pk,
    pv,
    qbuf,
    qf,
    acc,
    best,
    total,
    mate_acc,
    mate_best,
    mate_total,
    suf_acc,
    suf_best,
    suf_total,
    send_acc,
    send_stat,
    recv_acc,
    recv_stat,
    send_suf,
    send_sufstat,
    recv_suf,
    recv_sufstat,
    weight,
    pre_sem,
    suf_sem,
    q_send,
    q_recv,
    f_send,
    f_recv,
    m_send,
    m_recv,
    r_send,
    r_recv,
    u_send,
    u_recv,
):
    devices = kv_count * batch_count
    per_device, heads, dim = q_ref.shape
    local = heads // kv_count
    kv_local = local // group
    slots, rows, _ = sk_hbm.shape
    prefix_rows = pk_hbm.shape[0]
    prefix = prefix_rows // kv_local

    my_kv = lax.axis_index("kv")
    my_batch = lax.axis_index("batch")
    me = my_kv * batch_count + my_batch
    pairs = devices // 2
    core = lax.rem(me, 2)
    far = 1 - core
    my_pair = me // 2
    mate_place = (my_kv, my_batch + 1 - 2 * core)
    pair_rows = pairs * per_device

    pre_copies = [
        pltpu.make_async_copy(pk_hbm, pk_raw, pre_sem.at[0]),
        pltpu.make_async_copy(pv_hbm, pv_raw, pre_sem.at[1]),
    ]
    for copy in pre_copies:
        copy.start()

    def suffix_copies(slot):
        return (
            pltpu.make_async_copy(sk_hbm.at[slot], sk.at[slot], suf_sem.at[0, slot]),
            pltpu.make_async_copy(sv_hbm.at[slot], sv.at[slot], suf_sem.at[1, slot]),
        )

    for slot in range(slots):
        for copy in suffix_copies(slot):
            copy.start()

    barrier = pltpu.get_barrier_semaphore()

    def peer(step):
        other = lax.rem(me + step, devices)
        return other, (other // batch_count, lax.rem(other, batch_count))

    def greet(step, carry):
        _, place = peer(step)
        pl.semaphore_signal(barrier, inc=1, device_id=place, device_id_type=MESH)
        return carry

    lax.fori_loop(1, devices, greet, 0)
    pl.semaphore_wait(barrier, devices - 1)

    def send(src, dst, send_sem, recv_sem, place):
        return pltpu.make_async_remote_copy(
            src_ref=src,
            dst_ref=dst,
            send_sem=send_sem,
            recv_sem=recv_sem,
            device_id=place,
            device_id_type=MESH,
        )

    my_heads = pl.ds(pl.multiple_of(my_kv * local, local), local)

    def query_start(step, carry):
        other, place = peer(2 * step)
        heads_there = pl.ds(pl.multiple_of(place[0] * local, local), local)
        send(
            q_ref.at[:, heads_there, :], qbuf.at[my_pair, core], q_send.at[other // 2],
            q_recv.at[my_pair], place,
        ).start()
        return carry

    lax.fori_loop(1, pairs, query_start, 0)
    own_forward = send(
        q_ref.at[:, my_heads, :], qbuf.at[my_pair, core], f_send.at[my_pair], f_recv.at[my_pair],
        mate_place,
    )
    own_forward.start()
    qbuf[my_pair, core] = q_ref[:, my_heads, :]

    for copy, raw, parted in zip(pre_copies, (pk_raw, pv_raw), (pk, pv)):
        copy.wait()
        spread[...] = raw[...].astype(F32)
        for k in range(kv_local):
            parted[k] = spread[pl.ds(k, prefix, stride=kv_local), :].astype(BF16)

    def forward(pair):
        return send(
            qbuf.at[pair, core], qbuf.at[pair, core], f_send.at[pair], f_recv.at[pair], mate_place
        )

    def query_wait(step, carry):
        other, place = peer(2 * step)
        pair = other // 2
        arrived = qbuf.at[pair, core]
        send(arrived, arrived, q_send.at[pair], q_recv.at[pair], place).wait()
        forward(pair).start()
        return carry

    lax.fori_loop(1, pairs, query_wait, 0)

    contract_last = (((1,), (1,)), ((), ()))

    def attend_prefix(side):
        qf[...] = qbuf[:, side].astype(F32).reshape(pair_rows * local, dim)
        for k in range(kv_local):
            parts = [qf[pl.ds(k * group + j, pair_rows, stride=local), :] for j in range(group)]
            q = jnp.concatenate(parts, axis=0).astype(BF16)
            scores = lax.dot_general(q, pk[k], contract_last, preferred_element_type=F32) * scale
            row_best = jnp.max(scores, axis=-1, keepdims=True)
            weights = jnp.exp(scores - row_best)
            row_total = jnp.sum(weights, axis=-1, keepdims=True)
            row_acc = jnp.dot(weights.astype(BF16), pv[k], preferred_element_type=F32)
            wide_best = jnp.broadcast_to(row_best, row_acc.shape)
            wide_total = jnp.broadcast_to(row_total, row_acc.shape)
            for j in range(group):
                there = pl.ds(k * group + j, pair_rows, stride=local)
                here = slice(j * pair_rows, (j + 1) * pair_rows)
                acc[side, there, :] = row_acc[here]
                best[side, there, :] = wide_best[here]
                total[side, there, :] = wide_total[here]

    attend_prefix(core)

    def forward_wait(pair, carry):
        arrived = qbuf.at[pair, far]
        send(arrived, arrived, f_send.at[pair], f_recv.at[pair], mate_place).wait()
        return carry

    lax.fori_loop(0, pairs, forward_wait, 0)
    attend_prefix(far)

    mate_copies = [
        send(table.at[far], there, m_send.at[n], m_recv.at[n], mate_place)
        for n, (table, there) in enumerate(
            ((acc, mate_acc), (best, mate_best), (total, mate_total))
        )
    ]
    for copy in mate_copies:
        copy.start()

    column = lax.broadcasted_iota(jnp.int32, (local, rows), 1)
    head_row = lax.broadcasted_iota(jnp.int32, (local, rows), 0)
    own_head = lax.rem(column, kv_local) == head_row // group
    lane = lax.broadcasted_iota(jnp.int32, (local, dim), 1)
    sub = lax.broadcasted_iota(jnp.int32, (local, dim), 0)
    half = per_device * local

    def attend_suffix(slot):
        for copy in suffix_copies(slot):
            copy.wait()
        sequence = seq_ref[slot]
        owner = sequence // per_device
        q = qbuf[owner // 2, lax.rem(owner, 2), lax.rem(sequence, per_device)]
        scores = lax.dot_general(q, sk[slot], contract_last, preferred_element_type=F32) * scale
        live = own_head & (column < len_ref[slot] * kv_local)
        scores = jnp.where(live, scores, FILL)
        row_best = jnp.max(scores, axis=-1, keepdims=True)
        weights = jnp.exp(scores - row_best)
        row_total = jnp.sum(weights, axis=-1, keepdims=True)
        suf_acc[slot] = jnp.dot(weights.astype(BF16), sv[slot], preferred_element_type=F32)
        suf_best[slot] = jnp.broadcast_to(row_best, (local, dim))
        suf_total[slot] = jnp.broadcast_to(row_total, (local, dim))

    def mark(stat, w, new_best, new_total):
        stat = jnp.where(lane == sub + w * local, new_best, stat)
        return jnp.where(lane == sub + half + w * local, new_total, stat)

    def fold_pair(pair, acc_out, stat_out):
        stat = jnp.zeros((local, dim), F32)
        for w in range(per_device):
            table = pl.ds(pl.multiple_of((pair * per_device + w) * local, local), local)
            first_best = best[core, table, :]
            second_best = mate_best[table, :]
            new_best = jnp.maximum(first_best, second_best)
            first = jnp.exp(first_best - new_best)
            second = jnp.exp(second_best - new_best)
            new_total = total[core, table, :] * first + mate_total[table, :] * second
            new_acc = acc[core, table, :] * first + mate_acc[table, :] * second
            acc_out[w] = new_acc.astype(BF16)
            stat = mark(stat, w, new_best, new_total)
        stat_out[...] = jnp.sum(stat, axis=0, keepdims=True)

    def prefix_sends(step):
        other, place = peer(2 * step)
        pair = other // 2
        return pair, (
            send(send_acc.at[pair], recv_acc.at[my_pair], r_send.at[0, pair], r_recv.at[0, my_pair], place),
            send(send_stat.at[pair], recv_stat.at[my_pair], r_send.at[1, pair], r_recv.at[1, my_pair], place),
        )

    def prefix_start(step, carry):
        pair, copies = prefix_sends(step)
        fold_pair(pair, send_acc.at[pair], send_stat.at[pair])
        for copy in copies:
            copy.start()
        return carry

    def prefix_wait(step, carry):
        other, place = peer(2 * step)
        pair = other // 2
        send(send_acc.at[pair], recv_acc.at[pair], r_send.at[0, pair], r_recv.at[0, pair], place).wait()
        send(send_stat.at[pair], recv_stat.at[pair], r_send.at[1, pair], r_recv.at[1, pair], place).wait()
        return carry

    def pick_slot(other, acc_out, stat_out):
        at = jnp.int32(0)
        hits = []
        for w in range(per_device):
            hit = jnp.int32(0)
            for slot in range(slots):
                same = (seq_ref[slot] == other * per_device + w).astype(jnp.int32)
                at = jnp.maximum(at, same * slot)
                hit = jnp.maximum(hit, same)
            hits.append(hit)
        stat = jnp.zeros((local, dim), F32)
        for w in range(per_device):
            stat = mark(
                stat, w, jnp.where(hits[w] > 0, suf_best[at], FILL),
                jnp.where(hits[w] > 0, suf_total[at], 0.0),
            )
        acc_out[...] = suf_acc[at].astype(BF16)
        stat_out[...] = jnp.sum(stat, axis=0, keepdims=True)

    def suffix_start(step, carry):
        other, place = peer(step)
        pick_slot(other, send_suf.at[other], send_sufstat.at[other])
        send(send_suf.at[other], recv_suf.at[me], u_send.at[0, other], u_recv.at[0, me], place).start()
        send(send_sufstat.at[other], recv_sufstat.at[me], u_send.at[1, other], u_recv.at[1, me], place).start()
        return carry

    def suffix_wait(step, carry):
        other, place = peer(step)
        send(send_suf.at[other], recv_suf.at[other], u_send.at[0, other], u_recv.at[0, other], place).wait()
        send(send_sufstat.at[other], recv_sufstat.at[other], u_send.at[1, other], u_recv.at[1, other], place).wait()
        return carry

    early = slots // 2
    for slot in range(early):
        attend_suffix(slot)
    for copy in mate_copies:
        copy.wait()
    lax.fori_loop(1, pairs, prefix_start, 0)
    fold_pair(my_pair, recv_acc.at[my_pair], recv_stat.at[my_pair])
    for slot in range(early, slots):
        attend_suffix(slot)
    lax.fori_loop(1, devices, suffix_start, 0)
    pick_slot(me, recv_suf.at[me], recv_sufstat.at[me])
    lax.fori_loop(1, pairs, prefix_wait, 0)

    def column_of(row, w):
        picked = jnp.where(lane == sub + w * local, row, 0.0)
        return jnp.sum(picked, axis=-1, keepdims=True)

    def widen(values):
        return jnp.concatenate([values, jnp.zeros((values.shape[0], dim - half), F32)], axis=1)

    chips = batch_count // 2
    states = []
    for g in range(kv_count):
        stats = recv_stat[g * chips : (g + 1) * chips, 0, :]
        top = jnp.max(stats[:, :half], axis=0, keepdims=True)
        factor = jnp.exp(stats[:, :half] - top)
        denominator = jnp.sum(stats[:, half : 2 * half] * factor, axis=0, keepdims=True)
        weight[:chips, 0, :] = widen(factor)

        def add_prefix(index, sums, g=g):
            row = weight[index]
            return tuple(
                sums[w] + column_of(row, w) * recv_acc[g * chips + index, w].astype(F32)
                for w in range(per_device)
            )

        zeros = tuple(jnp.zeros((local, dim), F32) for _ in range(per_device))
        states.append((top, denominator, lax.fori_loop(0, chips, add_prefix, zeros, unroll=4)))

    lax.fori_loop(1, devices, suffix_wait, 0)
    for g in range(kv_count):
        top, denominator, sums = states[g]
        stats = recv_sufstat[g * batch_count : (g + 1) * batch_count, 0, :]
        new_top = jnp.maximum(top, jnp.max(stats[:, :half], axis=0, keepdims=True))
        factor = jnp.exp(stats[:, :half] - new_top)
        kept = jnp.exp(top - new_top)
        denominator = denominator * kept + jnp.sum(
            stats[:, half : 2 * half] * factor, axis=0, keepdims=True
        )
        weight[:batch_count, 0, :] = widen(factor / denominator)
        kept_row = widen(kept / denominator)
        sums = tuple(sums[w] * column_of(kept_row, w) for w in range(per_device))

        def add_suffix(index, sums, g=g):
            row = weight[index]
            part = recv_suf[g * batch_count + index].astype(F32)
            return tuple(sums[w] + column_of(row, w) * part for w in range(per_device))

        sums = lax.fori_loop(0, batch_count, add_suffix, sums, unroll=16)
        for w in range(per_device):
            out_ref[w, g * local : (g + 1) * local, :] = sums[w].astype(BF16)


def solution(mesh):
    kv_count = mesh.shape["kv"]
    batch_count = mesh.shape["batch"]
    devices = kv_count * batch_count

    def step(queries, prefix_keys, prefix_values, suffix_keys, suffix_values, lengths, slot_sequence):
        per_device, heads, dim = queries.shape
        local = heads // kv_count
        prefix, kv_local, _ = prefix_keys.shape
        slots, suffix, _, _ = suffix_keys.shape
        group = local // kv_local
        sequences = devices * per_device
        flat = sequences * local
        vmem = pl.BlockSpec(memory_space=pltpu.VMEM)
        smem = pl.BlockSpec(memory_space=pltpu.SMEM)
        hbm = pl.BlockSpec(memory_space=pl.ANY)
        dma = pltpu.SemaphoreType.DMA
        return pl.pallas_call(
            functools.partial(kernel, kv_count, batch_count, group, dim ** (-0.5)),
            out_shape=jax.ShapeDtypeStruct(queries.shape, BF16),
            in_specs=[smem, smem, vmem, hbm, hbm, hbm, hbm],
            out_specs=vmem,
            scratch_shapes=[
                pltpu.VMEM((prefix * kv_local, dim), BF16),
                pltpu.VMEM((prefix * kv_local, dim), BF16),
                pltpu.VMEM((slots, suffix * kv_local, dim), BF16),
                pltpu.VMEM((slots, suffix * kv_local, dim), BF16),
                pltpu.VMEM((prefix * kv_local, dim), F32),
                pltpu.VMEM((kv_local, prefix, dim), BF16),
                pltpu.VMEM((kv_local, prefix, dim), BF16),
                pltpu.VMEM((devices // 2, 2, per_device, local, dim), BF16),
                pltpu.VMEM((flat // 2, dim), F32),
                pltpu.VMEM((2, flat // 2, dim), F32),
                pltpu.VMEM((2, flat // 2, dim), F32),
                pltpu.VMEM((2, flat // 2, dim), F32),
                pltpu.VMEM((flat // 2, dim), F32),
                pltpu.VMEM((flat // 2, dim), F32),
                pltpu.VMEM((flat // 2, dim), F32),
                pltpu.VMEM((slots, local, dim), F32),
                pltpu.VMEM((slots, local, dim), F32),
                pltpu.VMEM((slots, local, dim), F32),
                pltpu.VMEM((devices // 2, per_device, local, dim), BF16),
                pltpu.VMEM((devices // 2, 1, dim), F32),
                pltpu.VMEM((devices // 2, per_device, local, dim), BF16),
                pltpu.VMEM((devices // 2, 1, dim), F32),
                pltpu.VMEM((devices, local, dim), BF16),
                pltpu.VMEM((devices, 1, dim), F32),
                pltpu.VMEM((devices, local, dim), BF16),
                pltpu.VMEM((devices, 1, dim), F32),
                pltpu.VMEM((devices, 1, dim), F32),
                dma((2,)),
                dma((2, slots)),
                dma((devices // 2,)),
                dma((devices // 2,)),
                dma((devices // 2,)),
                dma((devices // 2,)),
                dma((3,)),
                dma((3,)),
                dma((2, devices // 2)),
                dma((2, devices // 2)),
                dma((2, devices)),
                dma((2, devices)),
            ],
            compiler_params=pltpu.CompilerParams(
                collective_id=0, has_side_effects=True, vmem_limit_bytes=60 * 1024 * 1024
            ),
        )(
            slot_sequence,
            lengths,
            queries,
            prefix_keys.reshape(prefix * kv_local, dim),
            prefix_values.reshape(prefix * kv_local, dim),
            suffix_keys.reshape(slots, suffix * kv_local, dim),
            suffix_values.reshape(slots, suffix * kv_local, dim),
        )

    return jax.shard_map(
        step,
        mesh=mesh,
        in_specs=(
            P(("kv", "batch"), None, None),
            P("batch", "kv", None),
            P("batch", "kv", None),
            P("batch", None, "kv", None),
            P("batch", None, "kv", None),
            P("batch"),
            P("batch"),
        ),
        out_specs=P(("kv", "batch"), None, None),
        check_vma=False,
    )
```
